32 devices in a mesh: section: 2 (over x), dp: 16 (over z, y, core).
Axes of the slice: x: 2, y: 2, z: 4, core: 2. Of those that a mesh axis runs over, the one named last changes fastest.
Arguments:
- features: bfloat16 [1, 2, 2048, 4096], P(None, 'section', 'dp'), parts along dimension 2, may hold values from -6 to 6
- in_proj: bfloat16 [2, 4096, 512], P('section'), may hold values from -0.09375 to 0.09375
- mix_proj: bfloat16 [2, 2, 256, 256], P('section'), may hold values from -0.375 to 0.375
- out_proj: bfloat16 [2, 512, 4096], P('section'), may hold values from -0.375 to 0.375
- gate_proj: bfloat16 [2, 2, 4096], P('section'), may hold values from -0.09375 to 0.09375
- cross_bias: float32 [2, 4096], P('section'), may hold values from -3 to 3
Outputs:
- crossed: bfloat16 [1, 2, 2048, 4096], P(None, 'section', 'dp'), parts along dimension 2
The draws below stay inside these ranges and needn't reach their ends.
There are 16 independent parts, one for each index of `dp`. The reference program is written for one: setup_inputs(seed, part) draws one part's arguments, and reference() takes and returns one part's arrays. A program takes and returns all parts, laid end to end along the dimension named above; an argument that names none is the same for every part. Nothing has to cross between parts.
All inputs are finite; a program needn't handle non-finite values.
Results may differ from the reference program's by a relative error of at most 0.015.
Values may be sent and summed in bfloat16 or wider, within the bound.
No kernel may reach another device: no remote copies, remote signals or barrier semaphores. Data moves between devices by JAX's collectives and lax.ppermute only.
A program may use at most 64 MiB of HBM per device.

```python
import jax
import jax.numpy as jnp
from jax import lax

D = 4096
RANK = 256
EXPERTS = 2
ROWS = 128
MB_DEV = 1
LAYERS = 2
N_SECTION = 2


def shard_levels(own_key, shape, split, low, high):
    level = 1.0
    for dim, parts in split:
        steps = jax.random.uniform(jax.random.fold_in(jax.random.fold_in(own_key, 6), dim), (parts,), jnp.float32, low / len(split), high / len(split))
        level = level * jnp.repeat(jnp.exp(steps), shape[dim] // parts).reshape((-1,) + (1,) * (len(shape) - 1 - dim))
    return level


def centred(rng, extent, spread, reach, shards=(), kind=jnp.bfloat16):
    entries = spread * jax.random.normal(rng, extent, jnp.float32)
    if shards:
        entries = entries * shard_levels(rng, extent, shards, -0.22, 0.18)
    return jnp.clip(entries, -reach, reach).astype(kind)


def setup_inputs(seed: int = 0, part: int = 0) -> dict:
    arg_keys = jax.random.split(jax.random.key(seed), 7)
    part_splits = jax.random.split(jax.random.fold_in(arg_keys[6], part), 7)
    return {
        "features": centred(part_splits[0], (MB_DEV, N_SECTION, ROWS, D), 1.0, 6.0, ((1, 2),)),
        "in_proj": centred(arg_keys[1], (LAYERS, D, EXPERTS * RANK), D ** -0.5, 0.09375, ((0, 2),)),
        "mix_proj": centred(arg_keys[2], (LAYERS, EXPERTS, RANK, RANK), RANK ** -0.5, 0.375, ((0, 2),)),
        "out_proj": centred(arg_keys[3], (LAYERS, EXPERTS * RANK, D), RANK ** -0.5, 0.375, ((0, 2),)),
        "gate_proj": centred(arg_keys[4], (LAYERS, EXPERTS, D), D ** -0.5, 0.09375, ((0, 2),)),
        "cross_bias": centred(arg_keys[5], (LAYERS, D), 0.5, 3.0, ((0, 2),), jnp.float32),
    }


def cross_layer(current, anchor, v_mat, c_mat, u_mat, gate_mat, shift_row):
    row_count = current.shape[0]
    expert_count = c_mat.shape[0]
    rank_size = c_mat.shape[1]
    projected = jnp.dot(current, v_mat, preferred_element_type=jnp.float32)
    inner_first = jnp.tanh(projected).astype(jnp.bfloat16).reshape(row_count, expert_count, rank_size)
    inner_second = jnp.einsum("rek,ekj->rej", inner_first.astype(jnp.float32), c_mat.astype(jnp.float32))
    logits = lax.dot_general(current, gate_mat, (((1,), (1,)), ((), ())), preferred_element_type=jnp.float32)
    gate_values = 1.0 / jnp.sum(jnp.exp(logits[:, None, :] - logits[:, :, None]), axis=2)
    blended = (gate_values[:, :, None] * jnp.tanh(inner_second)).astype(jnp.bfloat16)
    blended = blended.reshape(row_count, expert_count * rank_size)
    crossed = jnp.dot(blended, u_mat, preferred_element_type=jnp.float32)
    updated = current.astype(jnp.float32) + anchor.astype(jnp.float32) * (crossed + shift_row)
    return updated.astype(jnp.bfloat16)


def reference(features, in_proj, mix_proj, out_proj, gate_proj, cross_bias):
    anchor = features.reshape(-1, features.shape[-1])
    current = anchor
    for level in range(LAYERS):
        current = cross_layer(current, anchor, in_proj[level], mix_proj[level], out_proj[level], gate_proj[level], cross_bias[level])
    return current.reshape(features.shape)
```

```python
import jax
import jax.numpy as jnp
from jax import lax
from jax.sharding import PartitionSpec as P


PIECES = 2


def from_behind(block, axis, distance):
    devices = range(lax.axis_size(axis))
    route = [(i - distance, i) for i in devices if i - distance in devices]
    return lax.ppermute(block, axis, route)


def blend(current, v_mat, c_mat, gate_mat):
    row_count = current.shape[0]
    expert_count = c_mat.shape[0]
    rank_size = c_mat.shape[1]
    projected = jnp.dot(current, v_mat, preferred_element_type=jnp.float32)
    inner_first = (
        jnp.tanh(projected).astype(jnp.bfloat16).reshape(row_count, expert_count, rank_size)
    )
    inner_second = jnp.einsum(
        "rek,ekj->rej", inner_first, c_mat, preferred_element_type=jnp.float32
    )
    logits = lax.dot_general(
        current, gate_mat, (((1,), (1,)), ((), ())), preferred_element_type=jnp.float32
    )
    gate_values = 1.0 / jnp.sum(jnp.exp(logits[:, None, :] - logits[:, :, None]), axis=2)
    blended = (gate_values[:, :, None] * jnp.tanh(inner_second)).astype(jnp.bfloat16)
    return blended.reshape(row_count, expert_count * rank_size)


def shifted_cross(blended, u_mat, shift_row):
    return jnp.dot(blended, u_mat, preferred_element_type=jnp.float32) + shift_row


def updated(current, anchor, moved):
    wide = current.astype(jnp.float32) + anchor.astype(jnp.float32) * moved.astype(jnp.float32)
    return wide.astype(jnp.bfloat16)


def cross_layer(current, anchor, v_mat, c_mat, u_mat, gate_mat, shift_row):
    blended = blend(current, v_mat, c_mat, gate_mat)
    return updated(current, anchor, shifted_cross(blended, u_mat, shift_row))


def relay_many(features, in_proj, mix_proj, out_proj, gate_proj, cross_bias):
    section_count = lax.axis_size("section")
    position = lax.axis_index("section")
    pieces = 1
    local_micro = features.shape[0]
    row_count = features.shape[2]
    feature_count = features.shape[3]
    piece_rows = row_count // pieces
    everyone = lax.all_gather(features, "section", axis=1, tiled=True)
    all_units = everyone.reshape(local_micro * section_count * pieces, piece_rows, feature_count)
    unit_count = all_units.shape[0]
    step_count = unit_count + section_count - 1
    v_mat = in_proj[0]
    c_mat = mix_proj[0]
    u_mat = out_proj[0]
    gate_mat = gate_proj[0]
    shift_row = cross_bias[0]

    def apply_layer(current, anchor):
        return cross_layer(current, anchor, v_mat, c_mat, u_mat, gate_mat, shift_row)

    def keep_input(current, anchor):
        return current

    def advance(carried, moment):
        incoming, outgoing, collected = carried
        unit_here = moment - position
        active = (unit_here >= 0) & (unit_here < unit_count)
        anchor = lax.dynamic_index_in_dim(
            all_units, jnp.clip(unit_here, 0, unit_count - 1), 0, keepdims=False
        )
        current = jnp.where(position == 0, anchor, incoming)
        result = lax.cond(active, apply_layer, keep_input, current, anchor)
        outgoing = jnp.where(position == section_count - 1, result, outgoing)
        held_unit = moment + position - 2 * section_count + 2
        arrived = (
            (held_unit >= 0)
            & (held_unit < unit_count)
            & (held_unit // pieces % section_count == position)
        )
        held_safe = jnp.clip(held_unit, 0, unit_count - 1)
        slot_index = held_safe // pieces // section_count * pieces + held_safe % pieces
        previous = lax.dynamic_index_in_dim(collected, slot_index, 0, keepdims=False)
        collected = lax.dynamic_update_index_in_dim(
            collected, jnp.where(arrived, outgoing, previous), slot_index, 0
        )
        return (result, outgoing, collected)

    def forward_step(carried, moment):
        result, outgoing, collected = advance(carried, moment)
        incoming = from_behind(result, "section", 1)
        return ((incoming, outgoing, collected), None)

    def cycle_step(carried, moment):
        moved, _ = forward_step(carried, moment)
        incoming, outgoing, collected = moved
        outgoing = from_behind(outgoing, "section", -1)
        return ((incoming, outgoing, collected), None)

    blank = jnp.zeros((piece_rows, feature_count), jnp.bfloat16)
    holding = jnp.zeros((local_micro * pieces, piece_rows, feature_count), jnp.bfloat16)
    carried, _ = lax.scan(
        forward_step, (blank, blank, holding), jnp.arange(0, section_count - 1, dtype=jnp.int32)
    )
    carried, _ = lax.scan(
        cycle_step, carried, jnp.arange(section_count - 1, step_count - 1, dtype=jnp.int32)
    )
    _, _, collected = advance(carried, jnp.int32(step_count - 1))
    return collected.reshape(local_micro, 1, row_count, feature_count)


def swap(block):
    return lax.ppermute(block, "section", [(0, 1), (1, 0)])


def pair_exchange(features, in_proj, mix_proj, out_proj, gate_proj, cross_bias):
    first_section = lax.axis_index("section") == 0
    local_micro, _, row_count, feature_count = features.shape
    rows = local_micro * row_count
    x0 = features.reshape(rows, feature_count)
    v_mat, c_mat, u_mat = in_proj[0], mix_proj[0], out_proj[0]
    gate_mat, shift_row = gate_proj[0], cross_bias[0]
    pieces = PIECES if rows % (16 * PIECES) == 0 else 1
    size = rows // pieces
    anchors = [x0[i * size : (i + 1) * size] for i in range(pieces)]
    sent, got = [], []
    for anchor in anchors:
        after = cross_layer(anchor, anchor, v_mat, c_mat, u_mat, gate_mat, shift_row)
        sent.append(jnp.where(first_section, after, anchor))
        got.append(swap(sent[-1]))
    back = []
    for block in got:
        moved = shifted_cross(blend(block, v_mat, c_mat, gate_mat), u_mat, shift_row)
        back.append(swap(moved.astype(jnp.bfloat16)))
    finished = []
    for anchor, current, moved in zip(anchors, sent, back):
        current = updated(current, anchor, moved)
        after = cross_layer(current, anchor, v_mat, c_mat, u_mat, gate_mat, shift_row)
        finished.append(jnp.where(first_section, current, after))
    return jnp.concatenate(finished, axis=0).reshape(features.shape)


def per_device(*arrays):
    if lax.axis_size("section") == 2:
        return pair_exchange(*arrays)
    return relay_many(*arrays)


def solution(mesh):
    placed = (
        P(None, "section", "dp", None),
        P("section", None, None),
        P("section", None, None, None),
        P("section", None, None),
        P("section", None, None),
        P("section", None),
    )
    return jax.shard_map(
        per_device,
        mesh=mesh,
        in_specs=placed,
        out_specs=P(None, "section", "dp", None),
        check_vma=False,
    )
```

```python
import jax
import jax.numpy as jnp
from jax import lax
from jax.sharding import PartitionSpec as P


CUTS = (6,13)


def from_behind(block, axis, distance):
    devices = range(lax.axis_size(axis))
    route = [(i - distance, i) for i in devices if i - distance in devices]
    return lax.ppermute(block, axis, route)


def blend(current, v_mat, c_mat, gate_mat):
    row_count = current.shape[0]
    expert_count = c_mat.shape[0]
    rank_size = c_mat.shape[1]
    projected = jnp.dot(current, v_mat, preferred_element_type=jnp.float32)
    inner_first = (
        jnp.tanh(projected).astype(jnp.bfloat16).reshape(row_count, expert_count, rank_size)
    )
    inner_second = jnp.einsum(
        "rek,ekj->rej", inner_first, c_mat, preferred_element_type=jnp.float32
    )
    logits = lax.dot_general(
        current, gate_mat, (((1,), (1,)), ((), ())), preferred_element_type=jnp.float32
    )
    gate_values = 1.0 / jnp.sum(jnp.exp(logits[:, None, :] - logits[:, :, None]), axis=2)
    blended = (gate_values[:, :, None] * jnp.tanh(inner_second)).astype(jnp.bfloat16)
    return blended.reshape(row_count, expert_count * rank_size)


def shifted_cross(blended, u_mat, shift_row):
    return jnp.dot(blended, u_mat, preferred_element_type=jnp.float32) + shift_row


def updated(current, anchor, moved):
    wide = current.astype(jnp.float32) + anchor.astype(jnp.float32) * moved.astype(jnp.float32)
    return wide.astype(jnp.bfloat16)


def cross_layer(current, anchor, v_mat, c_mat, u_mat, gate_mat, shift_row):
    blended = blend(current, v_mat, c_mat, gate_mat)
    return updated(current, anchor, shifted_cross(blended, u_mat, shift_row))


def relay_many(features, in_proj, mix_proj, out_proj, gate_proj, cross_bias):
    section_count = lax.axis_size("section")
    position = lax.axis_index("section")
    pieces = 1
    local_micro = features.shape[0]
    row_count = features.shape[2]
    feature_count = features.shape[3]
    piece_rows = row_count // pieces
    everyone = lax.all_gather(features, "section", axis=1, tiled=True)
    all_units = everyone.reshape(local_micro * section_count * pieces, piece_rows, feature_count)
    unit_count = all_units.shape[0]
    step_count = unit_count + section_count - 1
    v_mat = in_proj[0]
    c_mat = mix_proj[0]
    u_mat = out_proj[0]
    gate_mat = gate_proj[0]
    shift_row = cross_bias[0]

    def apply_layer(current, anchor):
        return cross_layer(current, anchor, v_mat, c_mat, u_mat, gate_mat, shift_row)

    def keep_input(current, anchor):
        return current

    def advance(carried, moment):
        incoming, outgoing, collected = carried
        unit_here = moment - position
        active = (unit_here >= 0) & (unit_here < unit_count)
        anchor = lax.dynamic_index_in_dim(
            all_units, jnp.clip(unit_here, 0, unit_count - 1), 0, keepdims=False
        )
        current = jnp.where(position == 0, anchor, incoming)
        result = lax.cond(active, apply_layer, keep_input, current, anchor)
        outgoing = jnp.where(position == section_count - 1, result, outgoing)
        held_unit = moment + position - 2 * section_count + 2
        arrived = (
            (held_unit >= 0)
            & (held_unit < unit_count)
            & (held_unit // pieces % section_count == position)
        )
        held_safe = jnp.clip(held_unit, 0, unit_count - 1)
        slot_index = held_safe // pieces // section_count * pieces + held_safe % pieces
        previous = lax.dynamic_index_in_dim(collected, slot_index, 0, keepdims=False)
        collected = lax.dynamic_update_index_in_dim(
            collected, jnp.where(arrived, outgoing, previous), slot_index, 0
        )
        return (result, outgoing, collected)

    def forward_step(carried, moment):
        result, outgoing, collected = advance(carried, moment)
        incoming = from_behind(result, "section", 1)
        return ((incoming, outgoing, collected), None)

    def cycle_step(carried, moment):
        moved, _ = forward_step(carried, moment)
        incoming, outgoing, collected = moved
        outgoing = from_behind(outgoing, "section", -1)
        return ((incoming, outgoing, collected), None)

    blank = jnp.zeros((piece_rows, feature_count), jnp.bfloat16)
    holding = jnp.zeros((local_micro * pieces, piece_rows, feature_count), jnp.bfloat16)
    carried, _ = lax.scan(
        forward_step, (blank, blank, holding), jnp.arange(0, section_count - 1, dtype=jnp.int32)
    )
    carried, _ = lax.scan(
        cycle_step, carried, jnp.arange(section_count - 1, step_count - 1, dtype=jnp.int32)
    )
    _, _, collected = advance(carried, jnp.int32(step_count - 1))
    return collected.reshape(local_micro, 1, row_count, feature_count)


def swap(block):
    return lax.ppermute(block, "section", [(0, 1), (1, 0)])


def pair_exchange(features, in_proj, mix_proj, out_proj, gate_proj, cross_bias):
    first_section = lax.axis_index("section") == 0
    local_micro, _, row_count, feature_count = features.shape
    rows = local_micro * row_count
    x0 = features.reshape(rows, feature_count)
    v_mat, c_mat, u_mat = in_proj[0], mix_proj[0], out_proj[0]
    gate_mat, shift_row = gate_proj[0], cross_bias[0]
    cuts = [0] + [rows * part // 16 // 8 * 8 for part in CUTS] + [rows]
    anchors = [x0[low:high] for low, high in zip(cuts, cuts[1:]) if high > low]
    sent, got = [], []
    for anchor in anchors:
        after = cross_layer(anchor, anchor, v_mat, c_mat, u_mat, gate_mat, shift_row)
        sent.append(jnp.where(first_section, after, anchor))
        got.append(swap(sent[-1]))
    back = []
    for block in got:
        moved = shifted_cross(blend(block, v_mat, c_mat, gate_mat), u_mat, shift_row)
        back.append(swap(moved.astype(jnp.bfloat16)))
    finished = []
    for anchor, current, moved in zip(anchors, sent, back):
        current = updated(current, anchor, moved)
        after = cross_layer(current, anchor, v_mat, c_mat, u_mat, gate_mat, shift_row)
        finished.append(jnp.where(first_section, current, after))
    return jnp.concatenate(finished, axis=0).reshape(features.shape)


def per_device(*arrays):
    if lax.axis_size("section") == 2:
        return pair_exchange(*arrays)
    return relay_many(*arrays)


def solution(mesh):
    placed = (
        P(None, "section", "dp", None),
        P("section", None, None),
        P("section", None, None, None),
        P("section", None, None),
        P("section", None, None),
        P("section", None),
    )
    return jax.shard_map(
        per_device,
        mesh=mesh,
        in_specs=placed,
        out_specs=P(None, "section", "dp", None),
        check_vma=False,
    )
```
